16 devices in a mesh: stage: 2 (over z), tp: 8 (over y, x, core).
Axes of the slice: x: 2, y: 2, z: 2, core: 2. Of those that a mesh axis runs over, the one named last changes fastest.
Arguments:
- x: bfloat16 [2, 2048, 4096], P(None, 'tp')
- g: bfloat16 [2, 2, 4096], P('stage')
- w1: bfloat16 [2, 2, 4096, 14336], P('stage', None, None, 'tp')
- w2: bfloat16 [2, 2, 14336, 4096], P('stage', None, 'tp')
Outputs:
- output: bfloat16 [2, 2, 2048, 4096], P('stage', None, 'tp')
All inputs are finite; a program needn't handle non-finite values.
Results may differ from the reference program's by a relative error of at most 0.0164811.
Values are sent between devices in bfloat16 or wider.
A program may use at most 1 GiB of HBM per device.

```python
import jax
import jax.numpy as jnp
from jax import lax

STAGES = 2
BLOCKS = 2
M = 2
T = 2048
D = 4096
FF = 14336

EPS = 1e-5


def setup_inputs(seed: int = 0) -> dict:
    k = jax.random.split(jax.random.key(seed), 4)
    x = jax.random.normal(k[0], (M, T, D), jnp.float32)
    g = 1.0 + 0.2 * jax.random.normal(k[1], (STAGES, BLOCKS, D), jnp.float32)
    w1 = jax.random.normal(k[2], (STAGES, BLOCKS, D, FF), jnp.float32) * D ** -0.5
    w2 = jax.random.normal(k[3], (STAGES, BLOCKS, FF, D), jnp.float32) * FF ** -0.5
    return {'x': x.astype(jnp.bfloat16), 'g': g.astype(jnp.bfloat16),
            'w1': w1.astype(jnp.bfloat16), 'w2': w2.astype(jnp.bfloat16)}


def _block(y, g, w1, w2):
    yf = y.astype(jnp.float32)
    mu = jnp.mean(yf, axis=-1, keepdims=True)
    var = jnp.mean(jnp.square(yf - mu), axis=-1, keepdims=True)
    h = ((yf - mu) * lax.rsqrt(var + EPS) * g.astype(jnp.float32)).astype(jnp.bfloat16)
    a = jax.nn.gelu(jnp.dot(h, w1, preferred_element_type=jnp.float32)).astype(jnp.bfloat16)
    return (yf + jnp.dot(a, w2, preferred_element_type=jnp.float32)).astype(jnp.bfloat16)


def reference(x, g, w1, w2):
    def one(xm):
        y = xm
        outs = []
        for s in range(STAGES):
            for b in range(BLOCKS):
                y = _block(y, g[s, b], w1[s, b], w2[s, b])
            outs.append(y)
        return jnp.stack(outs)
    return jnp.transpose(lax.map(one, x), (1, 0, 2, 3))
```

```python
import functools

import jax
import jax.numpy as jnp
from jax import lax
from jax.experimental import pallas as pl
from jax.experimental.pallas import tpu as pltpu
from jax.sharding import PartitionSpec as P

EPS = 1e-5
BF = jnp.bfloat16
F32 = jnp.float32
MESH = pl.DeviceIdType.MESH

CHUNKS = 16
NC = 4
TN1, TN2 = 256, 512
NB = 4


def _kernel(x_ref, g_ref, w1_ref, w2_ref, out_ref, ybuf, h8, p8, r0, r1, r2, abuf, w1b, w2b,
            ssem, rsem, zs, zr, osem, xsem, w1s, w2s):
    n, c, D = x_ref.shape
    nb, _, F = w1_ref.shape
    NT1, NT2 = F // TN1, D // TN2
    U = n * nb
    stage = lax.axis_index('stage')
    tp = lax.axis_index('tp')
    py, px, co = tp // 4, (tp // 2) % 2, tp % 2
    p1 = ((py + (1 - co) * (1 - 2 * py)) * 2 + px + co * (1 - 2 * px)) * 2 + co
    p2 = ((py + co * (1 - 2 * py)) * 2 + px + (1 - co) * (1 - 2 * px)) * 2 + co
    sib = (py * 2 + px) * 2 + 1 - co

    def unit(u):
        ctx = u % NC
        return ctx, (u // (nb * NC)) * NC + ctx, (u // NC) % nb

    def remote(src, dst, i, ctx, to):
        return pltpu.make_async_remote_copy(
            src_ref=src, dst_ref=dst, send_sem=ssem.at[i, ctx], recv_sem=rsem.at[i, ctx],
            device_id=(stage, to), device_id_type=MESH)

    def rows(ref, ctx, lo, hi):
        return ref.at[ctx, pl.ds(lo * c, (hi - lo) * c)]

    def ag1(x): return remote(rows(h8, x, 0, 1), rows(h8, x, 1, 2), 0, x, p1)
    def ag2(x): return remote(rows(h8, x, 0, 2), rows(h8, x, 2, 4), 1, x, p2)
    def ag3(x): return remote(rows(h8, x, 0, 4), rows(h8, x, 4, 8), 2, x, sib)
    def rs0(x): return remote(rows(p8, x, 4, 8), r0.at[x], 3, x, sib)
    def rs1(x): return remote(rows(p8, x, 2, 4), r1.at[x], 4, x, p2)
    def rs2(x): return remote(rows(p8, x, 1, 2), r2.at[x], 5, x, p1)

    def rs0_piece(x, t):
        cols = pl.ds(pl.multiple_of(t * TN2, TN2), TN2)
        return remote(p8.at[x, pl.ds(4 * c, 4 * c), cols], r0.at[x, :, cols], 3, x, sib)

    def zcopy(k):
        return pltpu.make_async_remote_copy(
            src_ref=ybuf.at[k], dst_ref=ybuf.at[k], send_sem=zs.at[k], recv_sem=zr.at[k],
            device_id=(1 - stage, tp), device_id_type=MESH)

    def ocopy(k):
        return pltpu.make_async_copy(ybuf.at[k], out_ref.at[k], osem.at[k])

    def w1copy(i):
        cols = pl.ds(pl.multiple_of((i % NT1) * TN1, TN1), TN1)
        return pltpu.make_async_copy(w1_ref.at[(i // (NT1 * NC)) % nb, :, cols], w1b.at[i % NB], w1s.at[i % NB])

    def w2copy(i):
        cols = pl.ds(pl.multiple_of((i % NT2) * TN2, TN2), TN2)
        return pltpu.make_async_copy(w2_ref.at[(i // (NT2 * NC)) % nb, :, cols], w2b.at[i % NB], w2s.at[i % NB])

    for i in range(NB - 1):
        w1copy(i).start()
        w2copy(i).start()

    @pl.when(stage == 0)
    def _():
        cp = pltpu.make_async_copy(x_ref, ybuf, xsem)
        cp.start()
        cp.wait()

    barrier = pltpu.get_barrier_semaphore()
    for to in ((stage, p1), (stage, p2), (stage, sib), (1 - stage, tp)):
        pl.semaphore_signal(barrier, inc=1, device_id=to, device_id_type=MESH)
    pl.semaphore_wait(barrier, 4)

    def ev_a(u):
        ctx, k, b = unit(u)

        @pl.when(jnp.logical_and(stage == 1, b == 0))
        def _():
            zcopy(k).wait_recv()
        yf = ybuf[k].astype(F32)
        mu = jnp.mean(yf, axis=-1, keepdims=True)
        yc = yf - mu
        var = jnp.mean(jnp.square(yc), axis=-1, keepdims=True)
        gb = g_ref[b].astype(F32)
        h8[ctx, pl.ds(0, c), :] = (yc * lax.rsqrt(var + EPS) * gb).astype(BF)
        ag1(ctx).start()

    def ev_b(u):
        ctx = unit(u)[0]
        ag1(ctx).wait()
        ag2(ctx).start()

    def ev_c(u):
        ctx = unit(u)[0]
        ag2(ctx).wait()
        ag3(ctx).start()

    def ev_e(u):
        ctx = unit(u)[0]
        rs0(ctx).wait()
        lo = pl.ds(2 * c, 2 * c)
        p8[ctx, lo, :] = (p8[ctx, lo, :].astype(F32) + r0[ctx, lo, :].astype(F32)).astype(BF)
        rs1(ctx).start()

    def ev_f(u):
        ctx = unit(u)[0]
        rs1(ctx).wait()
        lo = pl.ds(c, c)
        p8[ctx, lo, :] = (p8[ctx, lo, :].astype(F32) + r0[ctx, lo, :].astype(F32)
                          + r1[ctx, lo, :].astype(F32)).astype(BF)
        rs2(ctx).start()

    def ev_g(u):
        ctx, k, b = unit(u)
        rs2(ctx).wait()
        lo = pl.ds(0, c)
        ybuf[k] = (ybuf[k].astype(F32)
                   + (p8[ctx, lo, :].astype(F32) + r0[ctx, lo, :].astype(F32)
                      + r1[ctx, lo, :].astype(F32) + r2[ctx].astype(F32))).astype(BF)

        @pl.when(b == nb - 1)
        def _():
            ocopy(k).start()

            @pl.when(stage == 0)
            def _():
                zcopy(k).start()

    def guarded(f, u):
        @pl.when(jnp.logical_and(u >= 0, u < U))
        def _():
            f(u)

    def round_(step, carry):
        r = step - 2
        valid = jnp.logical_and(r >= 0, r < U)

        @pl.when(valid)
        def _():
            ag3(r % NC).wait()

        def t1(t, carry):
            @pl.when(valid)
            def _():
                i = r * NT1 + t
                ctx = r % NC

                @pl.when(i + NB - 1 < U * NT1)
                def _():
                    w1copy(i + NB - 1).start()
                w1copy(i).wait()
                z = jnp.dot(h8[ctx], w1b[i % NB], preferred_element_type=F32)
                abuf[:, pl.ds(pl.multiple_of(t * TN1, TN1), TN1)] = jax.nn.gelu(z).astype(BF)

            @pl.when(t == 1)
            def _():
                guarded(ev_e, r - 1)
                guarded(ev_g, r - 2)
                guarded(ev_a, r + 2)
                guarded(ev_c, r + 1)
            return carry

        lax.fori_loop(0, NT1, t1, 0)

        def t2(t, carry):
            @pl.when(valid)
            def _():
                i = r * NT2 + t
                ctx = r % NC

                @pl.when(i + NB - 1 < U * NT2)
                def _():
                    w2copy(i + NB - 1).start()
                w2copy(i).wait()
                z = jnp.dot(abuf[...], w2b[i % NB], preferred_element_type=F32)
                p8[ctx, :, pl.ds(pl.multiple_of(t * TN2, TN2), TN2)] = z.astype(BF)

                @pl.when(t > 0)
                def _():
                    rs0_piece(ctx, t - 1).start()

            @pl.when(t == 2)
            def _():
                guarded(ev_b, r + 2)
            return carry

        lax.fori_loop(0, NT2, t2, 0)

        @pl.when(valid)
        def _():
            rs0_piece(r % NC, NT2 - 1).start()
        guarded(ev_f, r - 1)
        return carry

    lax.fori_loop(0, U + 4, round_, 0)

    def drain(k, carry):
        ocopy(k).wait()

        @pl.when(stage == 0)
        def _():
            zcopy(k).wait_send()
        return carry

    lax.fori_loop(0, n, drain, 0)


def solution(mesh):
    def local(x, g, w1, w2):
        M, T, D = x.shape
        n = CHUNKS
        c = M * T // n
        F = w1.shape[-1]
        any_ = pl.BlockSpec(memory_space=pl.ANY)
        out = pl.pallas_call(
            _kernel,
            out_shape=jax.ShapeDtypeStruct((n, c, D), BF),
            in_specs=[any_, pl.BlockSpec(memory_space=pltpu.VMEM), any_, any_],
            out_specs=any_,
            scratch_shapes=[
                pltpu.VMEM((n, c, D), BF),
                pltpu.VMEM((NC, 8 * c, D), BF),
                pltpu.VMEM((NC, 8 * c, D), BF),
                pltpu.VMEM((NC, 4 * c, D), BF),
                pltpu.VMEM((NC, 2 * c, D), BF),
                pltpu.VMEM((NC, c, D), BF),
                pltpu.VMEM((8 * c, F), BF),
                pltpu.VMEM((NB, D, TN1), BF),
                pltpu.VMEM((NB, F, TN2), BF),
                pltpu.SemaphoreType.DMA((6, NC)),
                pltpu.SemaphoreType.DMA((6, NC)),
                pltpu.SemaphoreType.DMA((n,)),
                pltpu.SemaphoreType.DMA((n,)),
                pltpu.SemaphoreType.DMA((n,)),
                pltpu.SemaphoreType.DMA,
                pltpu.SemaphoreType.DMA((NB,)),
                pltpu.SemaphoreType.DMA((NB,)),
            ],
            compiler_params=pltpu.CompilerParams(
                collective_id=0, has_side_effects=True, vmem_limit_bytes=60 * 1024 * 1024),
        )(x.reshape(n, c, D), g[0][:, None], w1[0], w2[0])
        return out.reshape(1, M, T, D)

    return jax.shard_map(
        local, mesh=mesh,
        in_specs=(P(None, 'tp', None), P('stage', None, None),
                  P('stage', None, None, 'tp'), P('stage', None, 'tp', None)),
        out_specs=P('stage', None, 'tp', None), check_vma=False)
```

```python
import functools

import jax
import jax.numpy as jnp
from jax import lax
from jax.experimental import pallas as pl
from jax.experimental.pallas import tpu as pltpu
from jax.sharding import PartitionSpec as P

EPS = 1e-5
BF = jnp.bfloat16
F32 = jnp.float32
MESH = pl.DeviceIdType.MESH

CHUNKS = 16
NC = 4
TN1, TN2 = 256, 512
NB = 4
H = 2


def _kernel(x_ref, g_ref, w1_ref, w2_ref, out_ref, ybuf, h8, p8, r0, r1, r2, abuf, w1b, w2b,
            ssem, rsem, zs, zr, osem, xsem, w1s, w2s):
    n, c, D = x_ref.shape
    nb, _, F = w1_ref.shape
    NT1, NT2 = F // TN1, D // TN2
    U = n * nb
    DH = D // H
    stage = lax.axis_index('stage')
    tp = lax.axis_index('tp')
    py, px, co = tp // 4, (tp // 2) % 2, tp % 2
    p1 = ((py + (1 - co) * (1 - 2 * py)) * 2 + px + co * (1 - 2 * px)) * 2 + co
    p2 = ((py + co * (1 - 2 * py)) * 2 + px + (1 - co) * (1 - 2 * px)) * 2 + co
    sib = (py * 2 + px) * 2 + 1 - co

    def unit(u):
        ctx = u % NC
        return ctx, (u // (nb * NC)) * NC + ctx, (u // NC) % nb

    def remote(src, dst, i, ctx, to):
        return pltpu.make_async_remote_copy(
            src_ref=src, dst_ref=dst, send_sem=ssem.at[i, ctx], recv_sem=rsem.at[i, ctx],
            device_id=(stage, to), device_id_type=MESH)

    def part(ref, ctx, lo, hi, h):
        return ref.at[ctx, pl.ds(lo * c, (hi - lo) * c), pl.ds(h * DH, DH)]

    def ag1(x, h): return remote(part(h8, x, 0, 1, h), part(h8, x, 1, 2, h), h, x, p1)
    def ag2(x, h): return remote(part(h8, x, 0, 2, h), part(h8, x, 2, 4, h), 2 + h, x, p2)
    def ag3(x, h): return remote(part(h8, x, 0, 4, h), part(h8, x, 4, 8, h), 4 + h, x, sib)
    def rs0(x, h): return remote(part(p8, x, 4, 8, h), part(r0, x, 0, 4, h), 6 + h, x, sib)
    def rs1(x, h): return remote(part(p8, x, 2, 4, h), part(r1, x, 0, 2, h), 8 + h, x, p2)
    def rs2(x, h): return remote(part(p8, x, 1, 2, h), part(r2, x, 0, 1, h), 10 + h, x, p1)

    def rs0_piece(x, t):
        cols = pl.ds(pl.multiple_of(t * TN2, TN2), TN2)
        return remote(p8.at[x, pl.ds(4 * c, 4 * c), cols], r0.at[x, :, cols], 6 + t * TN2 // DH, x, sib)

    def zcopy(k, h):
        half = ybuf.at[k, :, pl.ds(h * DH, DH)]
        return pltpu.make_async_remote_copy(
            src_ref=half, dst_ref=half, send_sem=zs.at[k, h], recv_sem=zr.at[k, h],
            device_id=(1 - stage, tp), device_id_type=MESH)

    def ocopy(k, h):
        cols = pl.ds(h * DH, DH)
        return pltpu.make_async_copy(ybuf.at[k, :, cols], out_ref.at[k, :, cols], osem.at[k, h])

    def w1copy(i):
        cols = pl.ds(pl.multiple_of((i % NT1) * TN1, TN1), TN1)
        return pltpu.make_async_copy(w1_ref.at[(i // (NT1 * NC)) % nb, :, cols], w1b.at[i % NB], w1s.at[i % NB])

    def w2copy(i):
        cols = pl.ds(pl.multiple_of((i % NT2) * TN2, TN2), TN2)
        return pltpu.make_async_copy(w2_ref.at[(i // (NT2 * NC)) % nb, :, cols], w2b.at[i % NB], w2s.at[i % NB])

    for i in range(NB - 1):
        w1copy(i).start()
        w2copy(i).start()

    @pl.when(stage == 0)
    def _():
        cp = pltpu.make_async_copy(x_ref, ybuf, xsem)
        cp.start()
        cp.wait()

    barrier = pltpu.get_barrier_semaphore()
    for to in ((stage, p1), (stage, p2), (stage, sib), (1 - stage, tp)):
        pl.semaphore_signal(barrier, inc=1, device_id=to, device_id_type=MESH)
    pl.semaphore_wait(barrier, 4)

    def ev_a(u):
        ctx, k, b = unit(u)

        @pl.when(jnp.logical_and(stage == 1, b == 0))
        def _():
            for h in range(H):
                zcopy(k, h).wait_recv()
        yf = ybuf[k].astype(F32)
        mu = jnp.mean(yf, axis=-1, keepdims=True)
        yc = yf - mu
        var = jnp.mean(jnp.square(yc), axis=-1, keepdims=True)
        gb = g_ref[b].astype(F32)
        h8[ctx, pl.ds(0, c), :] = (yc * lax.rsqrt(var + EPS) * gb).astype(BF)
        for h in range(H):
            ag1(ctx, h).start()

    def ev_b(u, h):
        ctx = unit(u)[0]
        ag1(ctx, h).wait()
        ag2(ctx, h).start()

    def ev_c(u, h):
        ctx = unit(u)[0]
        ag2(ctx, h).wait()
        ag3(ctx, h).start()

    def ev_e(u, h):
        ctx = unit(u)[0]
        rs0(ctx, h).wait()
        at = (ctx, pl.ds(2 * c, 2 * c), pl.ds(h * DH, DH))
        p8[at] = (p8[at].astype(F32) + r0[at].astype(F32)).astype(BF)
        rs1(ctx, h).start()

    def ev_f(u, h):
        ctx = unit(u)[0]
        rs1(ctx, h).wait()
        at = (ctx, pl.ds(c, c), pl.ds(h * DH, DH))
        p8[at] = (p8[at].astype(F32) + r0[at].astype(F32) + r1[at].astype(F32)).astype(BF)
        rs2(ctx, h).start()

    def ev_g(u, h):
        ctx, k, b = unit(u)
        rs2(ctx, h).wait()
        at = (ctx, pl.ds(0, c), pl.ds(h * DH, DH))
        yat = (k, slice(None), pl.ds(h * DH, DH))
        ybuf[yat] = (ybuf[yat].astype(F32)
                     + (p8[at].astype(F32) + r0[at].astype(F32)
                        + r1[at].astype(F32) + r2[at].astype(F32))).astype(BF)

        @pl.when(b == nb - 1)
        def _():
            ocopy(k, h).start()

            @pl.when(stage == 0)
            def _():
                zcopy(k, h).start()

    def guarded(f, u, *h):
        @pl.when(jnp.logical_and(u >= 0, u < U))
        def _():
            f(u, *h)

    events = ((1, ev_g, -2, 1), (1, ev_a, 2), (1, ev_e, -1, 1), (2, ev_c, 1, 0),
              (7, ev_f, -1, 0), (7, ev_b, 2, 0), (10, ev_b, 2, 1), (10, ev_f, -1, 1), (11, ev_c, 1, 1),
              (12, ev_g, -1, 0), (13, ev_e, 0, 0))

    def run_events(r, base, steps, t):
        for p in sorted({e[0] for e in events if base <= e[0] < base + steps}):
            @pl.when(t == p - base)
            def _():
                for e in events:
                    if e[0] == p:
                        guarded(e[1], r + e[2], *e[3:])

    def round_(step, carry):
        r = step - 2
        valid = jnp.logical_and(r >= 0, r < U)

        @pl.when(valid)
        def _():
            for h in range(H):
                ag3(r % NC, h).wait()

        def t1(t, carry):
            @pl.when(valid)
            def _():
                i = r * NT1 + t
                ctx = r % NC

                @pl.when(i + NB - 1 < U * NT1)
                def _():
                    w1copy(i + NB - 1).start()
                w1copy(i).wait()
                z = jnp.dot(h8[ctx], w1b[i % NB], preferred_element_type=F32)
                abuf[:, pl.ds(pl.multiple_of(t * TN1, TN1), TN1)] = jax.nn.gelu(z).astype(BF)

            run_events(r, 0, NT1, t)
            return carry

        lax.fori_loop(0, NT1, t1, 0)

        def t2(t, carry):
            @pl.when(valid)
            def _():
                i = r * NT2 + t
                ctx = r % NC

                @pl.when(i + NB - 1 < U * NT2)
                def _():
                    w2copy(i + NB - 1).start()
                w2copy(i).wait()
                z = jnp.dot(abuf[...], w2b[i % NB], preferred_element_type=F32)
                p8[ctx, :, pl.ds(pl.multiple_of(t * TN2, TN2), TN2)] = z.astype(BF)

                @pl.when(t > 0)
                def _():
                    rs0_piece(ctx, t - 1).start()

            run_events(r, NT1, NT2, t)
            return carry

        lax.fori_loop(0, NT2, t2, 0)

        @pl.when(valid)
        def _():
            rs0_piece(r % NC, NT2 - 1).start()
        return carry

    lax.fori_loop(0, U + 4, round_, 0)

    def drain(k, carry):
        for h in range(H):
            ocopy(k, h).wait()

        @pl.when(stage == 0)
        def _():
            for h in range(H):
                zcopy(k, h).wait_send()
        return carry

    lax.fori_loop(0, n, drain, 0)


def solution(mesh):
    def local(x, g, w1, w2):
        M, T, D = x.shape
        n = CHUNKS
        c = M * T // n
        F = w1.shape[-1]
        any_ = pl.BlockSpec(memory_space=pl.ANY)
        out = pl.pallas_call(
            _kernel,
            out_shape=jax.ShapeDtypeStruct((n, c, D), BF),
            in_specs=[any_, pl.BlockSpec(memory_space=pltpu.VMEM), any_, any_],
            out_specs=any_,
            scratch_shapes=[
                pltpu.VMEM((n, c, D), BF),
                pltpu.VMEM((NC, 8 * c, D), BF),
                pltpu.VMEM((NC, 8 * c, D), BF),
                pltpu.VMEM((NC, 4 * c, D), BF),
                pltpu.VMEM((NC, 2 * c, D), BF),
                pltpu.VMEM((NC, c, D), BF),
                pltpu.VMEM((8 * c, F), BF),
                pltpu.VMEM((NB, D, TN1), BF),
                pltpu.VMEM((NB, F, TN2), BF),
                pltpu.SemaphoreType.DMA((6 * H, NC)),
                pltpu.SemaphoreType.DMA((6 * H, NC)),
                pltpu.SemaphoreType.DMA((n, H)),
                pltpu.SemaphoreType.DMA((n, H)),
                pltpu.SemaphoreType.DMA((n, H)),
                pltpu.SemaphoreType.DMA,
                pltpu.SemaphoreType.DMA((NB,)),
                pltpu.SemaphoreType.DMA((NB,)),
            ],
            compiler_params=pltpu.CompilerParams(
                collective_id=0, has_side_effects=True, vmem_limit_bytes=60 * 1024 * 1024),
        )(x.reshape(n, c, D), g[0][:, None], w1[0], w2[0])
        return out.reshape(1, M, T, D)

    return jax.shard_map(
        local, mesh=mesh,
        in_specs=(P(None, 'tp', None), P('stage', None, None),
                  P('stage', None, None, 'tp'), P('stage', None, 'tp', None)),
        out_specs=P('stage', None, 'tp', None), check_vma=False)
```

```python
import functools

import jax
import jax.numpy as jnp
from jax import lax
from jax.experimental import pallas as pl
from jax.experimental.pallas import tpu as pltpu
from jax.sharding import PartitionSpec as P

EPS = 1e-5
BF = jnp.bfloat16
F32 = jnp.float32
MESH = pl.DeviceIdType.MESH

CHUNKS = 16
NC = 4
TN1, TN2 = 256, 512
NB = 4
H = 2


def _kernel(x_ref, g_ref, w1_ref, w2_ref, out_ref, ybuf, h8, p8, r0, r1, r2, abuf, w1b, w2b,
            ssem, rsem, zs, zr, osem, xsem, w1s, w2s):
    n, c, D = x_ref.shape
    nb, _, F = w1_ref.shape
    NT1, NT2 = F // TN1, D // TN2
    U = n * nb
    DH = D // H
    stage = lax.axis_index('stage')
    tp = lax.axis_index('tp')
    py, px, co = tp // 4, (tp // 2) % 2, tp % 2
    p1 = ((py + (1 - co) * (1 - 2 * py)) * 2 + px + co * (1 - 2 * px)) * 2 + co
    p2 = ((py + co * (1 - 2 * py)) * 2 + px + (1 - co) * (1 - 2 * px)) * 2 + co
    sib = (py * 2 + px) * 2 + 1 - co

    def unit(u):
        ctx = u % NC
        return ctx, (u // (nb * NC)) * NC + ctx, (u // NC) % nb

    def remote(src, dst, i, ctx, to):
        return pltpu.make_async_remote_copy(
            src_ref=src, dst_ref=dst, send_sem=ssem.at[i, ctx], recv_sem=rsem.at[i, ctx],
            device_id=(stage, to), device_id_type=MESH)

    def part(ref, ctx, lo, hi, h):
        return ref.at[ctx, pl.ds(lo * c, (hi - lo) * c), pl.ds(h * DH, DH)]

    def ag1(x, h): return remote(part(h8, x, 0, 1, h), part(h8, x, 1, 2, h), h, x, p1)
    def ag2(x, h): return remote(part(h8, x, 0, 2, h), part(h8, x, 2, 4, h), 2 + h, x, p2)
    def ag3(x, h): return remote(part(h8, x, 0, 4, h), part(h8, x, 4, 8, h), 4 + h, x, sib)
    def rs0(x, h): return remote(part(p8, x, 4, 8, h), part(r0, x, 0, 4, h), 6 + h, x, sib)
    def rs1(x, h): return remote(part(p8, x, 2, 4, h), part(r1, x, 0, 2, h), 8 + h, x, p2)
    def rs2(x, h): return remote(part(p8, x, 1, 2, h), part(r2, x, 0, 1, h), 10 + h, x, p1)

    def rs0_piece(x, t):
        cols = pl.ds(pl.multiple_of(t * TN2, TN2), TN2)
        return remote(p8.at[x, pl.ds(4 * c, 4 * c), cols], r0.at[x, :, cols], 6 + t * TN2 // DH, x, sib)

    def zcopy(k, h):
        half = ybuf.at[k, :, pl.ds(h * DH, DH)]
        return pltpu.make_async_remote_copy(
            src_ref=half, dst_ref=half, send_sem=zs.at[k, h], recv_sem=zr.at[k, h],
            device_id=(1 - stage, tp), device_id_type=MESH)

    def ocopy(k, h):
        cols = pl.ds(h * DH, DH)
        return pltpu.make_async_copy(ybuf.at[k, :, cols], out_ref.at[k, :, cols], osem.at[k, h])

    def xcopy(k):
        return pltpu.make_async_copy(x_ref.at[k], ybuf.at[k], xsem.at[k])

    def w1copy(i):
        cols = pl.ds(pl.multiple_of((i % NT1) * TN1, TN1), TN1)
        return pltpu.make_async_copy(w1_ref.at[(i // (NT1 * NC)) % nb, :, cols], w1b.at[i % NB], w1s.at[i % NB])

    def w2copy(i):
        cols = pl.ds(pl.multiple_of((i % NT2) * TN2, TN2), TN2)
        return pltpu.make_async_copy(w2_ref.at[(i // (NT2 * NC)) % nb, :, cols], w2b.at[i % NB], w2s.at[i % NB])

    barrier = pltpu.get_barrier_semaphore()
    for to in ((stage, p1), (stage, p2), (stage, sib), (1 - stage, tp)):
        pl.semaphore_signal(barrier, inc=1, device_id=to, device_id_type=MESH)

    @pl.when(stage == 0)
    def _():
        for k in range(n):
            xcopy(k).start()
    for i in range(NB - 1):
        w1copy(i).start()
        w2copy(i).start()
    pl.semaphore_wait(barrier, 4)

    def ev_a(u):
        ctx, k, b = unit(u)

        @pl.when(jnp.logical_and(stage == 1, b == 0))
        def _():
            for h in range(H):
                zcopy(k, h).wait_recv()

        @pl.when(jnp.logical_and(stage == 0, b == 0))
        def _():
            xcopy(k).wait()
        yf = ybuf[k].astype(F32)
        mu = jnp.mean(yf, axis=-1, keepdims=True)
        yc = yf - mu
        var = jnp.mean(jnp.square(yc), axis=-1, keepdims=True)
        ga = g_ref[...].astype(F32)
        gb = ga[0:1]
        for i in range(1, nb):
            gb = jnp.where(b == i, ga[i:i + 1], gb)
        h8[ctx, pl.ds(0, c), :] = (yc * lax.rsqrt(var + EPS) * gb).astype(BF)
        for h in range(H):
            ag1(ctx, h).start()

    def ev_b(u, h):
        ctx = unit(u)[0]
        ag1(ctx, h).wait()
        ag2(ctx, h).start()

    def ev_c(u, h):
        ctx = unit(u)[0]
        ag2(ctx, h).wait()
        ag3(ctx, h).start()

    def ev_e(u, h):
        ctx = unit(u)[0]
        rs0(ctx, h).wait()
        at = (ctx, pl.ds(2 * c, 2 * c), pl.ds(h * DH, DH))
        p8[at] = (p8[at].astype(F32) + r0[at].astype(F32)).astype(BF)
        rs1(ctx, h).start()

    def ev_f(u, h):
        ctx = unit(u)[0]
        rs1(ctx, h).wait()
        at = (ctx, pl.ds(c, c), pl.ds(h * DH, DH))
        p8[at] = (p8[at].astype(F32) + r0[at].astype(F32) + r1[at].astype(F32)).astype(BF)
        rs2(ctx, h).start()

    def ev_g(u, h):
        ctx, k, b = unit(u)
        rs2(ctx, h).wait()
        at = (ctx, pl.ds(0, c), pl.ds(h * DH, DH))
        yat = (k, slice(None), pl.ds(h * DH, DH))
        ybuf[yat] = (ybuf[yat].astype(F32)
                     + (p8[at].astype(F32) + r0[at].astype(F32)
                        + r1[at].astype(F32) + r2[at].astype(F32))).astype(BF)

        @pl.when(b == nb - 1)
        def _():
            ocopy(k, h).start()

            @pl.when(stage == 0)
            def _():
                zcopy(k, h).start()

    def guarded(f, u, *h):
        @pl.when(jnp.logical_and(u >= 0, u < U))
        def _():
            f(u, *h)

    tables = (
        ((1, ev_e, -1, 1), (5, ev_b, 1, 1), (6, ev_c, 1, 0), (6, ev_f, -1, 0), (8, ev_f, -1, 1), (9, ev_a, 2),
         (12, ev_g, -1, 0), (12, ev_e, 0, 0), (13, ev_c, 1, 1), (13, ev_g, -1, 1), (14, ev_b, 2, 0)),
        ((0, ev_g, -3, 1), (0, ev_a, 1), (2, ev_f, -2, 1), (5, ev_b, 1, 0), (5, ev_b, 1, 1), (6, ev_e, -1, 1),
         (7, ev_g, -2, 0), (10, ev_f, -1, 0), (11, ev_c, 1, 0), (12, ev_e, 0, 0), (13, ev_c, 1, 1)))

    def run_events(r, base, steps, t):
        for st, events in enumerate(tables):
            for p in sorted({e[0] for e in events if base <= e[0] < base + steps}):
                @pl.when(jnp.logical_and(stage == st, t == p - base))
                def _():
                    for e in events:
                        if e[0] == p:
                            guarded(e[1], r + e[2], *e[3:])

    def round_(step, carry):
        r = step - 2
        valid = jnp.logical_and(r >= 0, r < U)

        @pl.when(valid)
        def _():
            for h in range(H):
                ag3(r % NC, h).wait()

        def t1(t, carry):
            @pl.when(valid)
            def _():
                i = r * NT1 + t
                ctx = r % NC

                @pl.when(i + NB - 1 < U * NT1)
                def _():
                    w1copy(i + NB - 1).start()
                w1copy(i).wait()
                z = jnp.dot(h8[ctx], w1b[i % NB], preferred_element_type=F32)
                abuf[:, pl.ds(pl.multiple_of(t * TN1, TN1), TN1)] = jax.nn.gelu(z).astype(BF)

            run_events(r, 0, NT1, t)
            return carry

        lax.fori_loop(0, NT1, t1, 0)

        def t2(t, carry):
            @pl.when(valid)
            def _():
                i = r * NT2 + t
                ctx = r % NC

                @pl.when(i + NB - 1 < U * NT2)
                def _():
                    w2copy(i + NB - 1).start()
                w2copy(i).wait()
                z = jnp.dot(abuf[...], w2b[i % NB], preferred_element_type=F32)
                p8[ctx, :, pl.ds(pl.multiple_of(t * TN2, TN2), TN2)] = z.astype(BF)

                @pl.when(t > 0)
                def _():
                    rs0_piece(ctx, t - 1).start()

            run_events(r, NT1, NT2, t)
            return carry

        lax.fori_loop(0, NT2, t2, 0)

        @pl.when(valid)
        def _():
            rs0_piece(r % NC, NT2 - 1).start()
        return carry

    lax.fori_loop(0, U + 5, round_, 0)

    def drain(k, carry):
        for h in range(H):
            ocopy(k, h).wait()

        @pl.when(stage == 0)
        def _():
            for h in range(H):
                zcopy(k, h).wait_send()
        return carry

    lax.fori_loop(0, n, drain, 0)


def solution(mesh):
    def local(x, g, w1, w2):
        M, T, D = x.shape
        n = CHUNKS
        c = M * T // n
        F = w1.shape[-1]
        any_ = pl.BlockSpec(memory_space=pl.ANY)
        out = pl.pallas_call(
            _kernel,
            out_shape=jax.ShapeDtypeStruct((n, c, D), BF),
            in_specs=[any_, pl.BlockSpec(memory_space=pltpu.VMEM), any_, any_],
            out_specs=any_,
            scratch_shapes=[
                pltpu.VMEM((n, c, D), BF),
                pltpu.VMEM((NC, 8 * c, D), BF),
                pltpu.VMEM((NC, 8 * c, D), BF),
                pltpu.VMEM((NC, 4 * c, D), BF),
                pltpu.VMEM((NC, 2 * c, D), BF),
                pltpu.VMEM((NC, c, D), BF),
                pltpu.VMEM((8 * c, F), BF),
                pltpu.VMEM((NB, D, TN1), BF),
                pltpu.VMEM((NB, F, TN2), BF),
                pltpu.SemaphoreType.DMA((6 * H, NC)),
                pltpu.SemaphoreType.DMA((6 * H, NC)),
                pltpu.SemaphoreType.DMA((n, H)),
                pltpu.SemaphoreType.DMA((n, H)),
                pltpu.SemaphoreType.DMA((n, H)),
                pltpu.SemaphoreType.DMA((n,)),
                pltpu.SemaphoreType.DMA((NB,)),
                pltpu.SemaphoreType.DMA((NB,)),
            ],
            compiler_params=pltpu.CompilerParams(
                collective_id=0, has_side_effects=True, vmem_limit_bytes=60 * 1024 * 1024),
        )(x.reshape(n, c, D), g[0], w1[0], w2[0])
        return out.reshape(1, M, T, D)

    return jax.shard_map(
        local, mesh=mesh,
        in_specs=(P(None, 'tp', None), P('stage', None, None),
                  P('stage', None, None, 'tp'), P('stage', None, 'tp', None)),
        out_specs=P('stage', None, 'tp', None), check_vma=False)
```

```python
import functools

import jax
import jax.numpy as jnp
from jax import lax
from jax.experimental import pallas as pl
from jax.experimental.pallas import tpu as pltpu
from jax.sharding import PartitionSpec as P

EPS = 1e-5
BF = jnp.bfloat16
F32 = jnp.float32
MESH = pl.DeviceIdType.MESH

CHUNKS = 16
NC = 4
TN1, TN2 = 256, 512
NB = 4
H = 2
LENT = 2


def _kernel(x_ref, g_ref, w1_ref, w2_ref, out_ref, ybuf, h8, p8, r0, r1, r2, abuf, w1b, w2b,
            ssem, rsem, zs, zr, osem, xsem, w1s, w2s, hz, gz, hs, hr, hx):
    n, c, D = x_ref.shape
    nb, _, F = w1_ref.shape
    NT1, NT2 = F // TN1, D // TN2
    U = n * nb
    DH = D // H
    stage = lax.axis_index('stage')
    tp = lax.axis_index('tp')
    py, px, co = tp // 4, (tp // 2) % 2, tp % 2
    p1 = ((py + (1 - co) * (1 - 2 * py)) * 2 + px + co * (1 - 2 * px)) * 2 + co
    p2 = ((py + co * (1 - 2 * py)) * 2 + px + (1 - co) * (1 - 2 * px)) * 2 + co
    sib = (py * 2 + px) * 2 + 1 - co

    def unit(u):
        ctx = u % NC
        return ctx, (u // (nb * NC)) * NC + ctx, (u // NC) % nb

    def remote(src, dst, i, ctx, to):
        return pltpu.make_async_remote_copy(
            src_ref=src, dst_ref=dst, send_sem=ssem.at[i, ctx], recv_sem=rsem.at[i, ctx],
            device_id=(stage, to), device_id_type=MESH)

    def part(ref, ctx, lo, hi, h):
        return ref.at[ctx, pl.ds(lo * c, (hi - lo) * c), pl.ds(h * DH, DH)]

    def ag1(x, h): return remote(part(h8, x, 0, 1, h), part(h8, x, 1, 2, h), h, x, p1)
    def ag2(x, h): return remote(part(h8, x, 0, 2, h), part(h8, x, 2, 4, h), 2 + h, x, p2)
    def ag3(x, h): return remote(part(h8, x, 0, 4, h), part(h8, x, 4, 8, h), 4 + h, x, sib)
    def rs0(x, h): return remote(part(p8, x, 4, 8, h), part(r0, x, 0, 4, h), 6 + h, x, sib)
    def rs1(x, h): return remote(part(p8, x, 2, 4, h), part(r1, x, 0, 2, h), 8 + h, x, p2)
    def rs2(x, h): return remote(part(p8, x, 1, 2, h), part(r2, x, 0, 1, h), 10 + h, x, p1)

    def rs0_piece(x, t):
        cols = pl.ds(pl.multiple_of(t * TN2, TN2), TN2)
        return remote(p8.at[x, pl.ds(4 * c, 4 * c), cols], r0.at[x, :, cols], 6 + t * TN2 // DH, x, sib)

    def zcopy(k, h):
        half = ybuf.at[k, :, pl.ds(h * DH, DH)]
        return pltpu.make_async_remote_copy(
            src_ref=half, dst_ref=half, send_sem=zs.at[k, h], recv_sem=zr.at[k, h],
            device_id=(1 - stage, tp), device_id_type=MESH)

    def ocopy(k, h):
        cols = pl.ds(h * DH, DH)
        return pltpu.make_async_copy(ybuf.at[k, :, cols], out_ref.at[k, :, cols], osem.at[k, h])

    def xcopy(k):
        return pltpu.make_async_copy(x_ref.at[k], ybuf.at[k], xsem.at[k])

    def lent(u):
        return jnp.logical_and(stage == 0, jnp.logical_and(u >= LENT, u < NC))

    def hcopy(j, i, h):
        src, dst, to = (
            (part(hz, i, 0, 1, h), part(hz, i, 1, 2, h), (stage, p1)),
            (part(hz, i, 0, 2, h), part(hz, i, 2, 4, h), (stage, p2)),
            (part(hz, i, 1, 4, h), part(h8, LENT + i, 1, 4, h), (1 - stage, tp)))[j]
        return pltpu.make_async_remote_copy(
            src_ref=src, dst_ref=dst, send_sem=hs.at[j * H + h, i], recv_sem=hr.at[j * H + h, i],
            device_id=to, device_id_type=MESH)

    def gcopy():
        return pltpu.make_async_remote_copy(
            src_ref=g_ref, dst_ref=gz, send_sem=hs.at[3 * H, 0], recv_sem=hr.at[3 * H, 0],
            device_id=(1 - stage, tp), device_id_type=MESH)

    def hxcopy(i):
        return pltpu.make_async_copy(x_ref.at[LENT + i], hz.at[i, pl.ds(0, c)], hx.at[i])

    def norm(y, gain):
        yf = y.astype(F32)
        yc = yf - jnp.mean(yf, axis=-1, keepdims=True)
        var = jnp.mean(jnp.square(yc), axis=-1, keepdims=True)
        return (yc * lax.rsqrt(var + EPS) * gain).astype(BF)

    def w1copy(i):
        cols = pl.ds(pl.multiple_of((i % NT1) * TN1, TN1), TN1)
        return pltpu.make_async_copy(w1_ref.at[(i // (NT1 * NC)) % nb, :, cols], w1b.at[i % NB], w1s.at[i % NB])

    def w2copy(i):
        cols = pl.ds(pl.multiple_of((i % NT2) * TN2, TN2), TN2)
        return pltpu.make_async_copy(w2_ref.at[(i // (NT2 * NC)) % nb, :, cols], w2b.at[i % NB], w2s.at[i % NB])

    barrier = pltpu.get_barrier_semaphore()
    for to in ((stage, p1), (stage, p2), (stage, sib), (1 - stage, tp)):
        pl.semaphore_signal(barrier, inc=1, device_id=to, device_id_type=MESH)

    @pl.when(stage == 0)
    def _():
        for k in range(n):
            xcopy(k).start()
    for i in range(NB - 1):
        w1copy(i).start()
        w2copy(i).start()
    pl.semaphore_wait(barrier, 4)

    @pl.when(stage == 0)
    def _():
        gcopy().start()

    @pl.when(stage == 1)
    def _():
        each = [(i, h) for i in range(NC - LENT) for h in range(H)]
        for i in range(NC - LENT):
            hxcopy(i).start()
        gcopy().wait_recv()
        gain = gz[...].astype(F32)[0:1]
        for i in range(NC - LENT):
            hxcopy(i).wait()
            hz[i, pl.ds(0, c), :] = norm(hz[i, pl.ds(0, c), :], gain)
            for h in range(H):
                hcopy(0, i, h).start()
        for j in (0, 1):
            for i, h in each:
                hcopy(j, i, h).wait()
                hcopy(j + 1, i, h).start()
        for i, h in each:
            hcopy(2, i, h).wait_send()

    def ev_a(u):
        ctx, k, b = unit(u)

        @pl.when(jnp.logical_and(stage == 1, b == 0))
        def _():
            for h in range(H):
                zcopy(k, h).wait_recv()

        @pl.when(jnp.logical_and(stage == 0, b == 0))
        def _():
            xcopy(k).wait()
        ga = g_ref[...].astype(F32)
        gb = ga[0:1]
        for i in range(1, nb):
            gb = jnp.where(b == i, ga[i:i + 1], gb)
        h8[ctx, pl.ds(0, c), :] = norm(ybuf[k], gb)

        @pl.when(jnp.logical_not(lent(u)))
        def _():
            for h in range(H):
                ag1(ctx, h).start()

    def ev_b(u, h):
        ctx = unit(u)[0]

        @pl.when(jnp.logical_not(lent(u)))
        def _():
            ag1(ctx, h).wait()
            ag2(ctx, h).start()

    def ev_c(u, h):
        ctx = unit(u)[0]

        @pl.when(jnp.logical_not(lent(u)))
        def _():
            ag2(ctx, h).wait()

        @pl.when(lent(u))
        def _():
            hcopy(2, u - LENT, h).wait_recv()
        ag3(ctx, h).start()

    def ev_e(u, h):
        ctx = unit(u)[0]
        rs0(ctx, h).wait()
        at = (ctx, pl.ds(2 * c, 2 * c), pl.ds(h * DH, DH))
        p8[at] = (p8[at].astype(F32) + r0[at].astype(F32)).astype(BF)
        rs1(ctx, h).start()

    def ev_f(u, h):
        ctx = unit(u)[0]
        rs1(ctx, h).wait()
        at = (ctx, pl.ds(c, c), pl.ds(h * DH, DH))
        p8[at] = (p8[at].astype(F32) + r0[at].astype(F32) + r1[at].astype(F32)).astype(BF)
        rs2(ctx, h).start()

    def ev_g(u, h):
        ctx, k, b = unit(u)
        rs2(ctx, h).wait()
        at = (ctx, pl.ds(0, c), pl.ds(h * DH, DH))
        yat = (k, slice(None), pl.ds(h * DH, DH))
        ybuf[yat] = (ybuf[yat].astype(F32)
                     + (p8[at].astype(F32) + r0[at].astype(F32)
                        + r1[at].astype(F32) + r2[at].astype(F32))).astype(BF)

        @pl.when(b == nb - 1)
        def _():
            ocopy(k, h).start()

            @pl.when(stage == 0)
            def _():
                zcopy(k, h).start()

    def guarded(f, u, *h):
        @pl.when(jnp.logical_and(u >= 0, u < U))
        def _():
            f(u, *h)

    tables = (
        ((1, ev_e, -1, 1), (5, ev_b, 1, 1), (6, ev_c, 1, 0), (6, ev_f, -1, 0), (8, ev_f, -1, 1), (9, ev_a, 2),
         (12, ev_g, -1, 0), (12, ev_e, 0, 0), (13, ev_c, 1, 1), (13, ev_g, -1, 1), (14, ev_b, 2, 0)),
        ((0, ev_g, -3, 1), (0, ev_a, 1), (2, ev_f, -2, 1), (5, ev_b, 1, 0), (5, ev_b, 1, 1), (6, ev_e, -1, 1),
         (7, ev_g, -2, 0), (10, ev_f, -1, 0), (11, ev_c, 1, 0), (12, ev_e, 0, 0), (13, ev_c, 1, 1)))

    def run_events(r, base, steps, t):
        for st, events in enumerate(tables):
            for p in sorted({e[0] for e in events if base <= e[0] < base + steps}):
                @pl.when(jnp.logical_and(stage == st, t == p - base))
                def _():
                    for e in events:
                        if e[0] == p:
                            guarded(e[1], r + e[2], *e[3:])

    def round_(step, carry):
        r = step - 2
        valid = jnp.logical_and(r >= 0, r < U)

        @pl.when(valid)
        def _():
            for h in range(H):
                ag3(r % NC, h).wait()

        def t1(t, carry):
            @pl.when(valid)
            def _():
                i = r * NT1 + t
                ctx = r % NC

                @pl.when(i + NB - 1 < U * NT1)
                def _():
                    w1copy(i + NB - 1).start()
                w1copy(i).wait()
                z = jnp.dot(h8[ctx], w1b[i % NB], preferred_element_type=F32)
                abuf[:, pl.ds(pl.multiple_of(t * TN1, TN1), TN1)] = jax.nn.gelu(z).astype(BF)

            run_events(r, 0, NT1, t)
            return carry

        lax.fori_loop(0, NT1, t1, 0)

        def t2(t, carry):
            @pl.when(valid)
            def _():
                i = r * NT2 + t
                ctx = r % NC

                @pl.when(i + NB - 1 < U * NT2)
                def _():
                    w2copy(i + NB - 1).start()
                w2copy(i).wait()
                z = jnp.dot(abuf[...], w2b[i % NB], preferred_element_type=F32)
                p8[ctx, :, pl.ds(pl.multiple_of(t * TN2, TN2), TN2)] = z.astype(BF)

                @pl.when(t > 0)
                def _():
                    rs0_piece(ctx, t - 1).start()

            run_events(r, NT1, NT2, t)
            return carry

        lax.fori_loop(0, NT2, t2, 0)

        @pl.when(valid)
        def _():
            rs0_piece(r % NC, NT2 - 1).start()
        return carry

    lax.fori_loop(0, U + 5, round_, 0)

    def drain(k, carry):
        for h in range(H):
            ocopy(k, h).wait()

        @pl.when(stage == 0)
        def _():
            for h in range(H):
                zcopy(k, h).wait_send()
        return carry

    lax.fori_loop(0, n, drain, 0)

    @pl.when(stage == 0)
    def _():
        gcopy().wait_send()


def solution(mesh):
    def local(x, g, w1, w2):
        M, T, D = x.shape
        n = CHUNKS
        c = M * T // n
        F = w1.shape[-1]
        any_ = pl.BlockSpec(memory_space=pl.ANY)
        out = pl.pallas_call(
            _kernel,
            out_shape=jax.ShapeDtypeStruct((n, c, D), BF),
            in_specs=[any_, pl.BlockSpec(memory_space=pltpu.VMEM), any_, any_],
            out_specs=any_,
            scratch_shapes=[
                pltpu.VMEM((n, c, D), BF),
                pltpu.VMEM((NC, 8 * c, D), BF),
                pltpu.VMEM((NC, 8 * c, D), BF),
                pltpu.VMEM((NC, 4 * c, D), BF),
                pltpu.VMEM((NC, 2 * c, D), BF),
                pltpu.VMEM((NC, c, D), BF),
                pltpu.VMEM((8 * c, F), BF),
                pltpu.VMEM((NB, D, TN1), BF),
                pltpu.VMEM((NB, F, TN2), BF),
                pltpu.SemaphoreType.DMA((6 * H, NC)),
                pltpu.SemaphoreType.DMA((6 * H, NC)),
                pltpu.SemaphoreType.DMA((n, H)),
                pltpu.SemaphoreType.DMA((n, H)),
                pltpu.SemaphoreType.DMA((n, H)),
                pltpu.SemaphoreType.DMA((n,)),
                pltpu.SemaphoreType.DMA((NB,)),
                pltpu.SemaphoreType.DMA((NB,)),
                pltpu.VMEM((NC - LENT, 4 * c, D), BF),
                pltpu.VMEM((g.shape[1], D), BF),
                pltpu.SemaphoreType.DMA((3 * H + 1, NC - LENT)),
                pltpu.SemaphoreType.DMA((3 * H + 1, NC - LENT)),
                pltpu.SemaphoreType.DMA((NC - LENT,)),
            ],
            compiler_params=pltpu.CompilerParams(
                collective_id=0, has_side_effects=True, vmem_limit_bytes=49 * 1024 * 1024),
        )(x.reshape(n, c, D), g[0], w1[0], w2[0])
        return out.reshape(1, M, T, D)

    return jax.shard_map(
        local, mesh=mesh,
        in_specs=(P(None, 'tp', None), P('stage', None, None),
                  P('stage', None, None, 'tp'), P('stage', None, 'tp', None)),
        out_specs=P('stage', None, 'tp', None), check_vma=False)
```
